256 devices in a mesh: samples: 64 (over z, y, x_hi), snps: 4 (over x_lo, core).
Axes of the slice: x: 4 (x_hi: 2, x_lo: 2; x = x_hi * 2 + x_lo), y: 4, z: 8, core: 2. Of those that a mesh axis runs over, the one named last changes fastest.
Arguments:
- genotype: int32 [32768, 1536], P('samples', 'snps'), may hold values from 0 to 2
- mask: int32 [32768, 1536], P('samples', 'snps'), may hold values 0 or 1
Outputs:
- blocks: float32 [32768, 16896], P('samples', 'snps')
The draws below stay inside these ranges and needn't reach their ends.
All inputs are finite; a program needn't handle non-finite values. No bound on the sum of `mask` on one device may be relied on, other than what follows from the above.
Results may differ from the reference program's by a relative error of at most 0.0014.
Values may be sent and summed in bfloat16 or wider, within the bound.
A program may use at most 128 MiB of HBM per device.

```python
import jax
import jax.numpy as jnp
from jax import lax

SNPS = 1536
SAMPLE_DEV = 512
SAMPLES = 32768
OFFSETS = 33
N_SAMPLES = 64


def draw_genotype(key, part):
    base_key = jax.random.fold_in(key, 11)
    key_percent = jax.random.fold_in(base_key, 1)
    key_first = jax.random.fold_in(base_key, 2)
    key_second = jax.random.fold_in(base_key, 3)
    percent = jax.random.randint(key_percent, (1, SNPS), 5, 31)
    sample_rows = lax.broadcasted_iota(jnp.int32, (SAMPLES, 1), 0)
    limit = percent * (SAMPLES + 2 * sample_rows)
    first_allele = jax.random.randint(key_first, (SAMPLES, SNPS), 0, 100) * SAMPLES
    second_allele = jax.random.randint(key_second, (SAMPLES, SNPS), 0, 100) * SAMPLES
    return (first_allele < limit).astype(jnp.int32) + (second_allele < limit).astype(jnp.int32)


def place_ends(values, rng, smallest, top_value):
    dims = values.shape
    place = [jax.random.randint(jax.random.fold_in(rng, axis), (), 0, dims[axis]) for axis in range(len(dims))]
    values = values.at[tuple(place)].set(smallest)
    longest = dims.index(max(dims))
    place[longest] = (place[longest] + 1) % dims[longest]
    return values.at[tuple(place)].set(top_value)


def setup_inputs(seed: int = 0) -> dict:
    splits = jax.random.split(jax.random.key(seed), 3)
    genotype = draw_genotype(jax.random.fold_in(splits[2], 71), 0)
    mask = place_ends((jax.random.randint(splits[1], (SAMPLES, SNPS), 0, 10) < 9).astype(jnp.int32), jax.random.fold_in(splits[1], 1), 0, 1)
    return dict(genotype=genotype, mask=mask)


def standardize(genotype, mask):
    dosage = genotype.astype(jnp.float32)
    observed_mask = mask.astype(jnp.float32)
    allele_sum = lax.optimization_barrier(jnp.sum(dosage * observed_mask, axis=0))
    observed_sum = lax.optimization_barrier(jnp.sum(observed_mask, axis=0))
    frequency = (allele_sum + 1.0) / (2.0 * observed_sum + 2.0)
    scaled = observed_mask * (dosage - 2.0 * frequency) / jnp.sqrt(2.0 * frequency * (1.0 - frequency))
    return scaled.astype(jnp.bfloat16)

def reference(genotype, mask):
    standard = standardize(genotype, mask)

    def block_row(block_index):
        begin = (block_index * SAMPLE_DEV).astype(jnp.int32)
        own_rows = lax.dynamic_slice_in_dim(standard, begin, SAMPLE_DEV, 0)
        rolled = jnp.roll(standard, -begin, axis=0)[:OFFSETS * SAMPLE_DEV]
        product = lax.dot_general(own_rows, rolled, (((1,), (1,)), ((), ())), preferred_element_type=jnp.float32)
        return product / SNPS
    result = lax.map(block_row, jnp.arange(N_SAMPLES, dtype=jnp.int32))
    return result.reshape(SAMPLES, OFFSETS * SAMPLE_DEV)
```

```python
import jax
import jax.numpy as jnp
from jax import lax
from jax.experimental import pallas as pl
from jax.experimental.pallas import tpu as pltpu
from jax.sharding import PartitionSpec as P

MESH = pl.DeviceIdType.MESH
Y = 4
R = 8
SLOTS = 5
TILE = 256


def sent_to_all(shard, axis):
    size = lax.axis_size(axis)
    return lax.all_to_all(
        jnp.broadcast_to(shard[None], (size, *shard.shape)), axis, 0, 0, tiled=True
    )


def packed_total(arrays, axis):
    flat = jnp.concatenate([a.reshape(-1) for a in arrays])
    running = sent_to_all(flat, axis).sum(axis=0)
    half = flat.shape[0] // 2
    return running[:half], running[half:]


def standardize(dosage, observed_mask, allele_sum, observed_sum):
    frequency = (allele_sum + 1.0) / (2.0 * observed_sum + 2.0)
    scaled = (
        observed_mask * (dosage - 2.0 * frequency) / jnp.sqrt(2.0 * frequency * (1.0 - frequency))
    )
    return scaled.astype(jnp.bfloat16)


def exchange_kernel(z_size, std, out, slots, lhs, stage, recv, recv_piece, recv_lhs, send, local_sem, out_sem):
    rows, width = std.shape
    total = 4 * width
    pair = 2 * rows
    chunk = rows // R
    i = lax.axis_index("samples")
    m = lax.axis_index("snps")
    xh, q = i % 2, i // 2
    y, z = q % Y, q // Y
    core, xl = m % 2, m // 2
    mine, theirs = xh, 1 - xh

    def at(dz, dy, half, member):
        zz = lax.rem(z + dz + z_size, z_size)
        yy = lax.rem(y + dy + Y, Y)
        return ((zz * Y + yy) * 2 + half, member)

    def span(slot, parity, r):
        return pl.ds(pl.multiple_of(slot * pair + parity * rows + r * chunk, chunk), chunk)

    def columns(member):
        return pl.ds(pl.multiple_of(member * width, width), width)

    def forward(stream, source, slot, parity, r, device):
        pltpu.make_async_remote_copy(
            src_ref=slots.at[span(source, parity, r)],
            dst_ref=slots.at[span(slot, parity, r)],
            send_sem=send.at[stream],
            recv_sem=recv.at[slot, parity, r],
            device_id=device,
            device_id_type=MESH,
        ).start()

    def arrived(slot, parity, r):
        pltpu.make_async_copy(
            slots.at[span(slot, parity, r)], slots.at[span(slot, parity, r)], recv.at[slot, parity, r]
        ).wait()

    def drained(stream, count):
        pltpu.make_async_copy(
            slots.at[pl.ds(0, count)], slots.at[pl.ds(0, count)], send.at[stream]
        ).wait()

    ring = [(h, k) for h in range(2) for k in range(4)]
    barrier = pltpu.get_barrier_semaphore()
    peers = []
    for dh in range(2):
        for dm in range(4):
            if dh or dm:
                peers.append(at(0, 0, lax.rem(xh + dh, 2), lax.rem(m + dm, 4)))
    for dz in (-1, 1):
        for c in range(2):
            peers.append(at(dz, 0, xh, xl * 2 + c))
    for dy in (-1, 1):
        peers.append(at(0, dy, xh, m))
    for peer in peers:
        pl.semaphore_signal(barrier, inc=1, device_id=peer, device_id_type=MESH)
    pl.semaphore_wait(barrier, len(peers))

    own_rows = pl.ds(pl.multiple_of(xh * rows, rows), rows)
    to_slot = pltpu.make_async_copy(std, slots.at[own_rows, columns(0)], local_sem)
    to_lhs = pltpu.make_async_copy(std, lhs.at[:, columns(m)], local_sem)

    @pl.when(m == 0)
    def _():
        to_slot.start()

    @pl.when(m != 0)
    def _():
        to_lhs.start()

        def piece(r, carry):
            pltpu.make_async_remote_copy(
                src_ref=std.at[pl.ds(pl.multiple_of(r * chunk, chunk), chunk)],
                dst_ref=slots.at[span(0, xh, r), columns(m)],
                send_sem=send.at[0],
                recv_sem=recv_piece.at[m, r],
                device_id=at(0, 0, xh, 0),
                device_id_type=MESH,
            ).start()
            return carry

        lax.fori_loop(0, R, piece, 0)

    def lhs_copy(dm):
        member = lax.rem(m + dm, 4)
        return pltpu.make_async_remote_copy(
            src_ref=std,
            dst_ref=lhs.at[:, columns(m)],
            send_sem=send.at[dm],
            recv_sem=recv_lhs.at[m],
            device_id=at(0, 0, xh, member),
            device_id_type=MESH,
        )

    def send_lhs():
        for dm in range(1, 4):
            @pl.when(lax.rem(m + dm, 4) != 0)
            def _():
                lhs_copy(dm).start()

    def both_ways(source, parity, r):
        forward(6, source, 3, parity, r, at(0, 1, xh, m))
        forward(7, source, 1, parity, r, at(0, -1, xh, m))

    def guarded(r, body):
        pl.when((r >= 0) & (r < R))(lambda: body(r))

    @pl.when(core == 0)
    def _():
        @pl.when(m == 0)
        def _():
            to_slot.wait()

        def own(r):
            @pl.when(xl == 0)
            def _():
                for member in range(1, 4):
                    pltpu.make_async_copy(
                        slots.at[span(0, xh, r), columns(member)],
                        slots.at[span(0, xh, r), columns(member)],
                        recv_piece.at[member, r],
                    ).wait()
                forward(4, 0, 0, mine, r, at(0, 0, 1 - xh, m))

            @pl.when(xl == 1)
            def _():
                arrived(0, mine, r)

            forward(5, 0, 0, mine, r, at(-1, 0, xh, m + 1))
            pl.when(y == Y - 1)(lambda: both_ways(0, mine, r))

        def other(r):
            arrived(0, theirs, r)
            pl.when(y == Y - 1)(lambda: both_ways(0, theirs, r))

        def last(r):
            for parity in (mine, theirs):
                arrived(4, parity, r)
                pl.when(y == 0)(lambda: both_ways(4, parity, r))

        def step(t, carry):
            guarded(t, own)
            guarded(t - 1, other)
            guarded(t - 2, last)
            return carry

        lax.fori_loop(0, R + 2, step, 0)
        send_lhs()

        def finish(r, carry):
            for slot in (1, 3, 2):
                for parity in (mine, theirs):
                    arrived(slot, parity, r)
            return carry

        lax.fori_loop(0, R, finish, 0)
        pl.when(xl == 0)(lambda: drained(4, rows))
        drained(5, rows)

        @pl.when((y == 0) | (y == Y - 1))
        def _():
            drained(6, pair)
            drained(7, pair)

    @pl.when(core == 1)
    def _():
        def first_out(parity, r):
            forward(6, 0, 4, parity, r, at(0, 0, xh, m - 1))
            pl.when(y > 0)(lambda: forward(8, 0, 1, parity, r, at(0, -1, xh, m)))
            pl.when(y == Y - 1)(lambda: forward(9, 0, 3, parity, r, at(0, 1, xh, m)))

        def last_out(parity, r):
            pl.when(y < Y - 1)(lambda: forward(9, 4, 3, parity, r, at(0, 1, xh, m)))
            pl.when(y == 0)(lambda: forward(8, 4, 1, parity, r, at(0, -1, xh, m)))

        def first_own(r):
            arrived(0, mine, r)
            forward(5, 0, 4, mine, r, at(-1, 0, xh, m))
            forward(4, 0, 0, mine, r, at(0, 0, 1 - xh, m))
            first_out(mine, r)

        def first_other(r):
            arrived(0, theirs, r)
            first_out(theirs, r)

        def last_own(r):
            arrived(4, mine, r)

            @pl.when(xl == 0)
            def _():
                forward(10, 4, 0, mine, r, at(0, 0, 0, 2))
                forward(11, 4, 0, mine, r, at(0, 0, 1, 2))

            forward(7, 4, 4, mine, r, at(0, 0, 1 - xh, m))
            last_out(mine, r)

        def last_other(r):
            arrived(4, theirs, r)
            last_out(theirs, r)

        def sides(r):
            for parity in (mine, theirs):
                arrived(1, parity, r)
                pl.when(y < 2)(lambda: forward(12, 1, 1, parity, r, at(1, 0, xh, m - 1)))
                pl.when((y == 1) | (y == 2))(lambda: forward(14, 1, 2, parity, r, at(0, -1, xh, m)))
                arrived(3, parity, r)
                pl.when(y >= 2)(lambda: forward(12, 3, 3, parity, r, at(1, 0, xh, m - 1)))
                pl.when((y == 1) | (y == 2))(lambda: forward(15, 3, 2, parity, r, at(0, 1, xh, m)))

        def middle(r):
            for parity in (mine, theirs):
                arrived(2, parity, r)
                forward(13, 2, 2, parity, r, at(1, 0, xh, m - 1))

        def step(t, carry):
            guarded(t, first_own)
            guarded(t - 1, first_other)
            guarded(t - 1, last_own)
            guarded(t - 2, last_other)
            guarded(t - 3, sides)
            guarded(t - 6, middle)
            return carry

        lax.fori_loop(0, R + 6, step, 0)
        send_lhs()
        for stream in (4, 5, 7):
            drained(stream, rows)
        for stream in (6, 8, 9, 12, 13):
            drained(stream, pair)

        @pl.when(xl == 0)
        def _():
            drained(10, rows)
            drained(11, rows)

        @pl.when((y == 1) | (y == 2))
        def _():
            drained(14, pair)
            drained(15, pair)

    @pl.when(m != 0)
    def _():
        to_lhs.wait()
        whole = std.at[:]
        pltpu.make_async_copy(whole, whole, send.at[0]).wait()
        for dm in range(1, 4):
            pltpu.make_async_copy(
                lhs.at[:, columns(lax.rem(m + dm, 4))],
                lhs.at[:, columns(lax.rem(m + dm, 4))],
                recv_lhs.at[lax.rem(m + dm, 4)],
            ).wait()

    for dm in range(1, 4):
        @pl.when(lax.rem(m + dm, 4) != 0)
        def _():
            lhs_copy(dm).wait_send()

    @pl.when(m == 0)
    def _():
        lhs[...] = slots[own_rows, :]

    begin = pl.multiple_of(xh * rows + m * (rows // 4), rows // 4)
    band = out.shape[1]

    def product(start, size):
        return lax.dot_general(
            lhs[...],
            slots[pl.ds(pl.multiple_of(begin + start, rows // 4), size), :],
            (((1,), (1,)), ((), ())),
            preferred_element_type=jnp.float32,
        )

    def to_out(k, slot):
        return pltpu.make_async_copy(
            stage.at[slot], out.at[:, pl.ds(pl.multiple_of(k * TILE, TILE), TILE)], out_sem.at[slot]
        )

    tiles = band // TILE

    def tile_step(k, carry):
        slot = lax.rem(k, 2)
        pl.when(k >= 2)(lambda: to_out(k - 2, slot).wait())
        stage[slot] = product(k * TILE, TILE)
        to_out(k, slot).start()
        return carry

    lax.fori_loop(0, tiles, tile_step, 0)
    to_out(tiles - 2, tiles % 2).wait()
    rest = band - tiles * TILE
    stage[tiles % 2, :, :rest] = product(tiles * TILE, rest)
    tail = pltpu.make_async_copy(
        stage.at[tiles % 2, :, pl.ds(0, rest)], out.at[:, pl.ds(tiles * TILE, rest)], out_sem.at[tiles % 2]
    )
    tail.start()
    to_out(tiles - 1, (tiles - 1) % 2).wait()
    tail.wait()


def per_device(genotype, mask):
    dosage = genotype.astype(jnp.float32)
    observed_mask = mask.astype(jnp.float32)
    allele_sum, observed_sum = packed_total(
        (jnp.sum(dosage * observed_mask, axis=0), jnp.sum(observed_mask, axis=0)), "samples"
    )
    standard = standardize(dosage, observed_mask, allele_sum, observed_sum)
    circle = lax.axis_size("samples")
    rows, width = standard.shape
    parts = lax.axis_size("snps")
    band = (circle // 2 + 1) * rows // parts
    total = width * parts

    def kernel(*refs):
        exchange_kernel(circle // (2 * Y), *refs)

    sums = pl.pallas_call(
        kernel,
        out_shape=jax.ShapeDtypeStruct((rows, band), jnp.float32),
        in_specs=[pl.BlockSpec(memory_space=pl.ANY)],
        out_specs=pl.BlockSpec(memory_space=pl.ANY),
        scratch_shapes=[
            pltpu.VMEM((SLOTS * 2 * rows, total), jnp.bfloat16),
            pltpu.VMEM((rows, total), jnp.bfloat16),
            pltpu.VMEM((2, rows, TILE), jnp.float32),
            pltpu.SemaphoreType.DMA((SLOTS, 2, R)),
            pltpu.SemaphoreType.DMA((4, R)),
            pltpu.SemaphoreType.DMA((4,)),
            pltpu.SemaphoreType.DMA((16,)),
            pltpu.SemaphoreType.DMA,
            pltpu.SemaphoreType.DMA((2,)),
        ],
        compiler_params=pltpu.CompilerParams(
            collective_id=0, has_side_effects=True, vmem_limit_bytes=48 * 1024 * 1024
        ),
        cost_estimate=pl.CostEstimate(
            flops=2 * rows * band * total, bytes_accessed=rows * band * 4, transcendentals=0
        ),
    )(standard)
    return sums / total


def solution(mesh):
    return jax.shard_map(
        per_device,
        mesh=mesh,
        in_specs=(P("samples", "snps"), P("samples", "snps")),
        out_specs=P("samples", "snps"),
        check_vma=False,
    )
```

```python
import jax
import jax.numpy as jnp
from jax import lax
from jax.experimental import pallas as pl
from jax.experimental.pallas import tpu as pltpu
from jax.sharding import PartitionSpec as P

MESH = pl.DeviceIdType.MESH
Y = 4
R = 16
SLOTS = 5
UNIT = 128
VMEM_MIB = 24


def standardize(dosage, observed_mask, allele_sum, observed_sum):
    frequency = (allele_sum + 1.0) / (2.0 * observed_sum + 2.0)
    scaled = (
        observed_mask * (dosage - 2.0 * frequency) / jnp.sqrt(2.0 * frequency * (1.0 - frequency))
    )
    return scaled.astype(jnp.bfloat16)


def exchange_kernel(
    z_size, genotype, mask, out,
    std, slots, lhs, plane, column, recv, recv_piece, recv_lhs, recv_count, send, send_count,
):
    rows, width = std.shape
    total = 4 * width
    pair = 2 * rows
    chunk = rows // R
    i = lax.axis_index("samples")
    m = lax.axis_index("snps")
    xh, q = i % 2, i // 2
    y, z = q % Y, q // Y
    core, xl = m % 2, m // 2
    mine, theirs = xh, 1 - xh
    band = out.shape[1]

    def at(dz, dy, half, member):
        zz = lax.rem(z + dz + z_size, z_size)
        yy = lax.rem(y + dy + Y, Y)
        return ((zz * Y + yy) * 2 + half, member)

    def span(slot, parity, r):
        return pl.ds(pl.multiple_of(slot * pair + parity * rows + r * chunk, chunk), chunk)

    def columns(member):
        return pl.ds(pl.multiple_of(member * width, width), width)

    def forward(stream, source, slot, parity, r, device):
        pltpu.make_async_remote_copy(
            src_ref=slots.at[span(source, parity, r)],
            dst_ref=slots.at[span(slot, parity, r)],
            send_sem=send.at[stream],
            recv_sem=recv.at[slot, parity, r],
            device_id=device,
            device_id_type=MESH,
        ).start()

    def arrived(slot, parity, r):
        pltpu.make_async_copy(
            slots.at[span(slot, parity, r)], slots.at[span(slot, parity, r)], recv.at[slot, parity, r]
        ).wait()

    def drained(stream, count):
        pltpu.make_async_copy(
            slots.at[pl.ds(0, count)], slots.at[pl.ds(0, count)], send.at[stream]
        ).wait()

    ring = [(h, k) for h in range(2) for k in range(4)]
    barrier = pltpu.get_barrier_semaphore()
    peers = []
    for dh in range(2):
        for dm in range(4):
            if dh or dm:
                peers.append(at(0, 0, lax.rem(xh + dh, 2), lax.rem(m + dm, 4)))
    for dz in (-1, 1):
        for c in range(2):
            peers.append(at(dz, 0, xh, xl * 2 + c))
    for dy in (-1, 1):
        peers.append(at(0, dy, xh, m))
    here = y * 2 + xh
    crowd = []
    for d in range(1, 2 * Y):
        other = lax.rem(here + d, 2 * Y)
        crowd.append((i - here + other, m))
    tower = [at(d, 0, xh, m) for d in range(1, z_size)]
    everyone = peers + crowd + tower
    for peer in everyone:
        pl.semaphore_signal(barrier, inc=1, device_id=peer, device_id_type=MESH)

    def counted(ref_a, ref_b):
        dosage, seen = ref_a[...].astype(jnp.float32), ref_b[...].astype(jnp.float32)
        return (
            jnp.sum(dosage * seen, axis=0, keepdims=True),
            jnp.sum(seen, axis=0, keepdims=True),
        )

    alleles, observed = counted(genotype, mask)
    line = lax.broadcasted_iota(jnp.int32, (8, width), 0)
    plane[here] = jnp.where(line == 0, alleles, jnp.where(line == 1, observed, 0.0))
    pl.semaphore_wait(barrier, len(everyone))

    def share(buffer, index, phase, devices, size):
        copies = [
            pltpu.make_async_remote_copy(
                src_ref=buffer.at[index],
                dst_ref=buffer.at[index],
                send_sem=send_count.at[phase, d],
                recv_sem=recv_count.at[phase, index],
                device_id=device,
                device_id_type=MESH,
            )
            for d, device in enumerate(devices)
        ]
        for copy in copies:
            copy.start()
        for d in range(1, size):
            source = lax.rem(index + d, size)
            pltpu.make_async_copy(
                buffer.at[source], buffer.at[source], recv_count.at[phase, source]
            ).wait()
        return copies

    sent = share(plane, here, 0, crowd, 2 * Y)
    column[z] = jnp.sum(plane[...], axis=0)
    sent += share(column, z, 1, tower, z_size)
    counts = jnp.sum(column[...], axis=0)
    standard = standardize(
        genotype[...].astype(jnp.float32), mask[...].astype(jnp.float32), counts[0:1], counts[1:2]
    )
    std[...] = standard
    own_rows = pl.ds(pl.multiple_of(xh * rows, rows), rows)

    @pl.when(m == 0)
    def _():
        slots[own_rows, 0:width] = standard

    for member in range(1, 4):
        @pl.when(m == member)
        def _():
            lhs[:, member * width : (member + 1) * width] = standard

    @pl.when(m != 0)
    def _():
        def piece(r, carry):
            pltpu.make_async_remote_copy(
                src_ref=std.at[pl.ds(pl.multiple_of(r * chunk, chunk), chunk)],
                dst_ref=slots.at[span(0, xh, r), columns(m)],
                send_sem=send.at[0],
                recv_sem=recv_piece.at[m, r],
                device_id=at(0, 0, xh, 0),
                device_id_type=MESH,
            ).start()
            return carry

        lax.fori_loop(0, R, piece, 0)

    def lhs_copy(stream, source, owner, member):
        return pltpu.make_async_remote_copy(
            src_ref=source,
            dst_ref=lhs.at[:, columns(owner)],
            send_sem=send.at[stream],
            recv_sem=recv_lhs.at[owner],
            device_id=at(0, 0, xh, member),
            device_id_type=MESH,
        )

    mate = jnp.where(m < 2, m + 2, 5 - m)
    lhs_copy(1, std, m, mate).start()
    pl.when(m != 1)(lambda: lhs_copy(2, std, m, 1).start())

    def lhs_wait(owner):
        pltpu.make_async_copy(
            lhs.at[:, columns(owner)], lhs.at[:, columns(owner)], recv_lhs.at[owner]
        ).wait()

    def pass_lhs():
        @pl.when(m >= 2)
        def _():
            lhs_wait(m - 2)
            lhs_copy(3, lhs.at[:, columns(m - 2)], m - 2, 5 - m).start()

    def lhs_ready():
        @pl.when(m == 0)
        def _():
            lhs[...] = slots[own_rows, :]

        @pl.when(m == 1)
        def _():
            for owner in (0, 2, 3):
                lhs_wait(owner)

        @pl.when(m >= 2)
        def _():
            lhs_wait(5 - m)
            lhs_wait(3 - m)

    begin = xh * 4 + m

    def product(unit, count):
        first = pl.multiple_of(unit * UNIT, UNIT)
        out[:, pl.ds(pl.multiple_of((unit - begin) * UNIT, UNIT), count * UNIT)] = lax.dot_general(
            lhs[...],
            slots[pl.ds(first, count * UNIT), :],
            (((1,), (1,)), ((), ())),
            preferred_element_type=jnp.float32,
        )

    def tile(slot, parity, half):
        unit = slot * (pair // UNIT) + parity * (rows // UNIT) + half * 2
        low = unit - begin
        units = band // UNIT
        pl.when((low >= 0) & (low < units - 1))(lambda: product(unit, 2))
        pl.when(low == -1)(lambda: product(unit + 1, 1))
        pl.when(low == units - 1)(lambda: product(unit, 1))

    def both_ways(source, parity, r):
        forward(6, source, 3, parity, r, at(0, 1, xh, m))
        forward(7, source, 1, parity, r, at(0, -1, xh, m))

    def guarded(r, body):
        pl.when((r >= 0) & (r < R))(lambda: body(r))

    @pl.when(core == 0)
    def _():
        def own(r):
            @pl.when(xl == 0)
            def _():
                for member in range(1, 4):
                    pltpu.make_async_copy(
                        slots.at[span(0, xh, r), columns(member)],
                        slots.at[span(0, xh, r), columns(member)],
                        recv_piece.at[member, r],
                    ).wait()
                forward(4, 0, 0, mine, r, at(0, 0, 1 - xh, m))

            @pl.when(xl == 1)
            def _():
                arrived(0, mine, r)

            forward(5, 0, 0, mine, r, at(-1, 0, xh, m + 1))
            pl.when(y == Y - 1)(lambda: both_ways(0, mine, r))

        def other(r):
            arrived(0, theirs, r)
            pl.when(y == Y - 1)(lambda: both_ways(0, theirs, r))

        def last(r):
            for parity in (mine, theirs):
                arrived(4, parity, r)
                pl.when(y == 0)(lambda: both_ways(4, parity, r))

        def step(t, carry):
            guarded(t, own)
            guarded(t - 1, other)
            guarded(t - 2, last)
            pl.when(t == 1)(pass_lhs)
            return carry

        lax.fori_loop(0, R + 2, step, 0)
        lhs_ready()

        def finish(half, carry):
            for slot in (0, 4, 1, 3, 2):
                for parity in (mine, theirs):
                    if slot in (1, 2, 3):
                        def chunks(r, c):
                            arrived(slot, parity, half * (R // 2) + r)
                            return c

                        lax.fori_loop(0, R // 2, chunks, 0)
                    tile(slot, parity, half)
            return carry

        lax.fori_loop(0, 2, finish, 0)
        pl.when(xl == 0)(lambda: drained(4, rows))
        drained(5, rows)

        @pl.when((y == 0) | (y == Y - 1))
        def _():
            drained(6, pair)
            drained(7, pair)

    @pl.when(core == 1)
    def _():
        def first_out(parity, r):
            forward(6, 0, 4, parity, r, at(0, 0, xh, m - 1))
            pl.when(y > 0)(lambda: forward(8, 0, 1, parity, r, at(0, -1, xh, m)))
            pl.when(y == Y - 1)(lambda: forward(9, 0, 3, parity, r, at(0, 1, xh, m)))

        def last_out(parity, r):
            pl.when(y < Y - 1)(lambda: forward(9, 4, 3, parity, r, at(0, 1, xh, m)))
            pl.when(y == 0)(lambda: forward(8, 4, 1, parity, r, at(0, -1, xh, m)))

        def first_own(r):
            arrived(0, mine, r)
            forward(5, 0, 4, mine, r, at(-1, 0, xh, m))
            forward(4, 0, 0, mine, r, at(0, 0, 1 - xh, m))
            first_out(mine, r)

        def first_other(r):
            arrived(0, theirs, r)
            first_out(theirs, r)

        def last_own(r):
            arrived(4, mine, r)

            @pl.when(xl == 0)
            def _():
                forward(10, 4, 0, mine, r, at(0, 0, 0, 2))
                forward(11, 4, 0, mine, r, at(0, 0, 1, 2))

            forward(7, 4, 4, mine, r, at(0, 0, 1 - xh, m))
            last_out(mine, r)

        def last_other(r):
            arrived(4, theirs, r)
            last_out(theirs, r)

        def sides(r):
            for parity in (mine, theirs):
                arrived(1, parity, r)
                pl.when(y < 2)(lambda: forward(12, 1, 1, parity, r, at(1, 0, xh, m - 1)))
                pl.when((y == 1) | (y == 2))(lambda: forward(14, 1, 2, parity, r, at(0, -1, xh, m)))
                arrived(3, parity, r)
                pl.when(y >= 2)(lambda: forward(12, 3, 3, parity, r, at(1, 0, xh, m - 1)))
                pl.when((y == 1) | (y == 2))(lambda: forward(15, 3, 2, parity, r, at(0, 1, xh, m)))

        def middle(r):
            for parity in (mine, theirs):
                arrived(2, parity, r)
                forward(13, 2, 2, parity, r, at(1, 0, xh, m - 1))

        def early_tile(k, half):
            slot = jnp.where(k < 2, 0, jnp.where(k < 4, 4, jnp.where(k < 6, 1, jnp.where(k < 8, 3, 2))))
            tile(slot, jnp.where(k % 2 == 0, mine, theirs), half)

        def step(t, carry):
            guarded(t, first_own)
            guarded(t - 1, first_other)
            guarded(t - 1, last_own)
            guarded(t - 2, last_other)
            guarded(t - 3, sides)
            guarded(t - 4, middle)

            pl.when(t == 1)(pass_lhs)
            pl.when(t == R // 2)(lhs_ready)
            pl.when((t >= R // 2) & (t < R // 2 + 10))(lambda: early_tile(t - R // 2, 0))
            return carry

        lax.fori_loop(0, R + 4, step, 0)

        def late(k, carry):
            early_tile(k, 1)
            return carry

        lax.fori_loop(0, 10, late, 0)
        for stream in (4, 5, 7):
            drained(stream, rows)
        for stream in (6, 8, 9, 12, 13):
            drained(stream, pair)

        @pl.when(xl == 0)
        def _():
            drained(10, rows)
            drained(11, rows)

        @pl.when((y == 1) | (y == 2))
        def _():
            drained(14, pair)
            drained(15, pair)

    for copy in sent:
        copy.wait_send()
    lhs_copy(1, std, m, mate).wait_send()
    pl.when(m != 1)(lambda: lhs_copy(2, std, m, 1).wait_send())
    pl.when(m >= 2)(lambda: lhs_copy(3, std, m - 2, 5 - m).wait_send())
    pl.when(m != 0)(lambda: pltpu.make_async_copy(std, std, send.at[0]).wait())


def per_device(genotype, mask):
    circle = lax.axis_size("samples")
    rows, width = genotype.shape
    parts = lax.axis_size("snps")
    band = (circle // 2 + 1) * rows // parts
    total = width * parts
    z_size = circle // (2 * Y)

    def kernel(*refs):
        exchange_kernel(z_size, *refs)

    sums = pl.pallas_call(
        kernel,
        out_shape=jax.ShapeDtypeStruct((rows, band), jnp.float32),
        in_specs=[pl.BlockSpec(memory_space=pltpu.VMEM)] * 2,
        out_specs=pl.BlockSpec(memory_space=pltpu.VMEM),
        scratch_shapes=[
            pltpu.VMEM((rows, width), jnp.bfloat16),
            pltpu.VMEM((SLOTS * 2 * rows, total), jnp.bfloat16),
            pltpu.VMEM((rows, total), jnp.bfloat16),
            pltpu.VMEM((2 * Y, 8, width), jnp.float32),
            pltpu.VMEM((z_size, 8, width), jnp.float32),
            pltpu.SemaphoreType.DMA((SLOTS, 2, R)),
            pltpu.SemaphoreType.DMA((4, R)),
            pltpu.SemaphoreType.DMA((4,)),
            pltpu.SemaphoreType.DMA((2, max(z_size, 2 * Y))),
            pltpu.SemaphoreType.DMA((16,)),
            pltpu.SemaphoreType.DMA((2, max(z_size, 2 * Y))),
        ],
        compiler_params=pltpu.CompilerParams(
            collective_id=0, has_side_effects=True, vmem_limit_bytes=VMEM_MIB * 1024 * 1024
        ),
        cost_estimate=pl.CostEstimate(
            flops=2 * rows * band * total, bytes_accessed=rows * band * 4, transcendentals=0
        ),
    )(genotype, mask)
    return sums / total


def solution(mesh):
    return jax.shard_map(
        per_device,
        mesh=mesh,
        in_specs=(P("samples", "snps"), P("samples", "snps")),
        out_specs=P("samples", "snps"),
        check_vma=False,
    )
```

```python
import jax
import jax.numpy as jnp
from jax import lax
from jax.experimental import pallas as pl
from jax.experimental.pallas import tpu as pltpu
from jax.sharding import PartitionSpec as P

MESH = pl.DeviceIdType.MESH
Y = 4
R = 16
SLOTS = 5
UNIT = 128
DOUBLED = (3, 3)
CROSSED = (3, 2)
MID_CROSSED = (0, 4)
FIRST_DOWN = (4, 3)
LAST_DOWN = (4, 2)
LAG_EVEN = ((0, 2, 12), (0, 2, 15))
LAG_ODD = ((0, 1, 4, 5, 7), (0, 2, 4, 4, 6))
VMEM_MIB = 30


def levels(allele_sum, observed_sum):
    frequency = (allele_sum + 1.0) / (2.0 * observed_sum + 2.0)
    spread = jnp.sqrt(2.0 * frequency * (1.0 - frequency))
    return [(dosage - 2.0 * frequency) / spread for dosage in (0.0, 1.0, 2.0)]


def exchange_kernel(
    z_size, call, out,
    std, slots, lhs, plane, column, recv, recv_piece, recv_lhs, recv_count, send, send_count,
):
    rows, width = std.shape
    total = 4 * width
    pair = 2 * rows
    chunk = rows // R
    i = lax.axis_index("samples")
    m = lax.axis_index("snps")
    xh, q = i % 2, i // 2
    y, z = q % Y, q // Y
    core, xl = m % 2, m // 2
    mine, theirs = xh, 1 - xh
    band = out.shape[1]

    def at(dz, dy, half, member):
        zz = lax.rem(z + dz + z_size, z_size)
        yy = lax.rem(y + dy + Y, Y)
        return ((zz * Y + yy) * 2 + half, member)

    def span(slot, parity, r):
        return pl.ds(pl.multiple_of(slot * pair + parity * rows + r * chunk, chunk), chunk)

    def columns(member):
        return pl.ds(pl.multiple_of(member * width, width), width)

    def forward(stream, source, slot, parity, r, device):
        pltpu.make_async_remote_copy(
            src_ref=slots.at[span(source, parity, r)],
            dst_ref=slots.at[span(slot, parity, r)],
            send_sem=send.at[stream],
            recv_sem=recv.at[slot, parity, r],
            device_id=device,
            device_id_type=MESH,
        ).start()

    def arrived(slot, parity, r):
        pltpu.make_async_copy(
            slots.at[span(slot, parity, r)], slots.at[span(slot, parity, r)], recv.at[slot, parity, r]
        ).wait()

    def drained(stream, count):
        pltpu.make_async_copy(
            slots.at[pl.ds(0, count)], slots.at[pl.ds(0, count)], send.at[stream]
        ).wait()

    barrier = pltpu.get_barrier_semaphore()
    peers = []
    for dh in range(2):
        for dm in range(4):
            if dh or dm:
                peers.append(at(0, 0, lax.rem(xh + dh, 2), lax.rem(m + dm, 4)))
    for dz in (-1, 1):
        for c in range(2):
            peers.append(at(dz, 0, xh, xl * 2 + c))
    for dy in (-1, 1):
        peers.append(at(0, dy, xh, m))
    here = y * 2 + xh
    crowd = []
    for d in range(1, 2 * Y):
        other = lax.rem(here + d, 2 * Y)
        crowd.append((i - here + other, m))
    tower = [at(d, 0, xh, m) for d in range(1, z_size)]
    everyone = peers + crowd + tower
    for peer in everyone:
        pl.semaphore_signal(barrier, inc=1, device_id=peer, device_id_type=MESH)

    value = call[...].astype(jnp.float32)
    lanes = width // 3
    sums = (
        jnp.sum(jnp.maximum(value - 1.0, 0.0), axis=0, keepdims=True),
        jnp.sum(jnp.minimum(value, 1.0), axis=0, keepdims=True),
    )
    line = lax.broadcasted_iota(jnp.int32, (8, lanes), 0)
    packed = jnp.zeros((8, lanes), jnp.float32)
    for k in range(6):
        part = sums[k // 3][:, (k % 3) * lanes : (k % 3 + 1) * lanes]
        packed = jnp.where(line == k, part, packed)
    plane[here] = packed
    pl.semaphore_wait(barrier, len(everyone))

    def share(buffer, index, phase, devices, size):
        copies = [
            pltpu.make_async_remote_copy(
                src_ref=buffer.at[index],
                dst_ref=buffer.at[index],
                send_sem=send_count.at[phase, d],
                recv_sem=recv_count.at[phase, index],
                device_id=device,
                device_id_type=MESH,
            )
            for d, device in enumerate(devices)
        ]
        for copy in copies:
            copy.start()
        for d in range(1, size):
            source = lax.rem(index + d, size)
            pltpu.make_async_copy(
                buffer.at[source], buffer.at[source], recv_count.at[phase, source]
            ).wait()
        return copies

    sent = share(plane, here, 0, crowd, 2 * Y)
    column[z] = jnp.sum(plane[...], axis=0)
    sent += share(column, z, 1, tower, z_size)
    counts = jnp.sum(column[...], axis=0)
    alleles, observed = (
        jnp.concatenate([counts[3 * k + n : 3 * k + n + 1] for n in range(3)], axis=1) for k in range(2)
    )
    low, middle_level, high = levels(alleles, observed)
    seen = jnp.where(value == 1.0, low, jnp.where(value == 2.0, middle_level, high))
    standard = jnp.where(value == 0.0, 0.0, seen).astype(jnp.bfloat16)
    std[...] = standard
    own_rows = pl.ds(pl.multiple_of(xh * rows, rows), rows)

    @pl.when(m == 0)
    def _():
        slots[own_rows, 0:width] = standard

    for member in range(1, 4):
        @pl.when(m == member)
        def _():
            lhs[:, member * width : (member + 1) * width] = standard

    @pl.when(m != 0)
    def _():
        def piece(r, carry):
            pltpu.make_async_remote_copy(
                src_ref=std.at[pl.ds(pl.multiple_of(r * chunk, chunk), chunk)],
                dst_ref=slots.at[span(0, xh, r), columns(m)],
                send_sem=send.at[0],
                recv_sem=recv_piece.at[m, r],
                device_id=at(0, 0, xh, 0),
                device_id_type=MESH,
            ).start()
            return carry

        lax.fori_loop(0, R, piece, 0)

    def lhs_copy(stream, source, owner, member):
        return pltpu.make_async_remote_copy(
            src_ref=source,
            dst_ref=lhs.at[:, columns(owner)],
            send_sem=send.at[stream],
            recv_sem=recv_lhs.at[owner],
            device_id=at(0, 0, xh, member),
            device_id_type=MESH,
        )

    mate = jnp.where(m < 2, m + 2, 5 - m)
    lhs_copy(1, std, m, mate).start()
    pl.when(m != 1)(lambda: lhs_copy(2, std, m, 1).start())

    def lhs_wait(owner):
        pltpu.make_async_copy(
            lhs.at[:, columns(owner)], lhs.at[:, columns(owner)], recv_lhs.at[owner]
        ).wait()

    def pass_lhs():
        @pl.when(m >= 2)
        def _():
            lhs_wait(m - 2)
            lhs_copy(3, lhs.at[:, columns(m - 2)], m - 2, 5 - m).start()

    def lhs_ready():
        @pl.when(m == 0)
        def _():
            lhs[...] = slots[own_rows, :]

        @pl.when(m == 1)
        def _():
            for owner in (0, 2, 3):
                lhs_wait(owner)

        @pl.when(m >= 2)
        def _():
            lhs_wait(5 - m)
            lhs_wait(3 - m)

    begin = xh * 4 + m

    def product(unit, count):
        first = pl.multiple_of(unit * UNIT, UNIT)
        out[:, pl.ds(pl.multiple_of((unit - begin) * UNIT, UNIT), count * UNIT)] = lax.dot_general(
            lhs[...],
            slots[pl.ds(first, count * UNIT), :],
            (((1,), (1,)), ((), ())),
            preferred_element_type=jnp.float32,
        ) / total

    def tile(slot, parity, half):
        unit = slot * (pair // UNIT) + parity * (rows // UNIT) + half * 2
        low = unit - begin
        units = band // UNIT
        pl.when((low >= 0) & (low < units - 1))(lambda: product(unit, 2))
        pl.when(low == -1)(lambda: product(unit + 1, 1))
        pl.when(low == units - 1)(lambda: product(unit, 1))

    def by_half(values):
        return values[0] if values[0] == values[1] else jnp.where(xl == 0, values[0], values[1])

    def marked(shares, shift, r):
        return lax.rem(r + shift, 4) < by_half(shares)

    def doubled(r):
        return marked(DOUBLED, 0, r)

    def crossed(r):
        return marked(CROSSED, 1, r)

    def mid_crossed(r):
        return marked(MID_CROSSED, 2, r)

    def guarded(n, body):
        @pl.when((n >= 0) & (n < 2 * R))
        def _():
            own = n < R
            body(own, jnp.where(own, mine, theirs), lax.rem(n, R))

    def both_ways(source, parity, r):
        forward(6, source, 3, parity, r, at(0, 1, xh, m))
        forward(7, source, 1, parity, r, at(0, -1, xh, m))

    def tiles_of(k, group, start=0, stop=4):
        j, phase = lax.rem(k, R // 2), k // (R // 2)

        @pl.when((k >= 0) & (phase >= start) & (phase < stop) & (j < len(group)))
        def _():
            slot = jnp.int32(group[-1])
            for place, value in enumerate(group[:-1]):
                slot = jnp.where(j == place, value, slot)
            tile(slot, jnp.where(phase < 2, mine, theirs), lax.rem(phase, 2))

    def tile_step(t, early, late, whole):
        pl.when(t == early + (R if whole else R // 2))(lhs_ready)
        tiles_of(t - early - R // 2, (0, 4), start=int(whole))
        if whole:
            tiles_of(t - early - R - 2, (0, 4), stop=1)
        tiles_of(t - late - R // 2, (1, 3, 2))

    def settle(stream, count):
        for half in range(2):
            if count(half):
                pl.when(xl == half)(lambda: drained(stream, chunk * count(half)))

    def tally(shares, shift):
        return lambda half: [int((r + shift) % 4 < shares[half]) for r in range(R)]

    is_doubled, is_crossed, is_mid = tally(DOUBLED, 0), tally(CROSSED, 1), tally(MID_CROSSED, 2)
    is_first, is_last = tally(FIRST_DOWN, 3), tally(LAST_DOWN, 1)
    steps = 2 * R
    side = jnp.where(y < 2, 3, 1)

    @pl.when(core == 0)
    def _():
        def first(own, parity, r):
            @pl.when(own & (xl == 0))
            def _():
                for member in range(1, 4):
                    pltpu.make_async_copy(
                        slots.at[span(0, xh, r), columns(member)],
                        slots.at[span(0, xh, r), columns(member)],
                        recv_piece.at[member, r],
                    ).wait()
                forward(4, 0, 0, mine, r, at(0, 0, 1 - xh, m))

            @pl.when(jnp.logical_not(own & (xl == 0)))
            def _():
                arrived(0, parity, r)

            pl.when(own | marked(FIRST_DOWN, 3, r))(
                lambda: forward(5, 0, 0, parity, r, at(-1, 0, xh, m + 1))
            )
            pl.when((y == Y - 1) & doubled(r))(lambda: both_ways(0, parity, r))

        def last(own, parity, r):
            arrived(4, parity, r)
            pl.when((y == 0) & doubled(r))(lambda: both_ways(4, parity, r))

        def sides(own, parity, r):
            for slot in (1, 3, 2):
                arrived(slot, parity, r)
                by_ring = doubled(r) & (side == slot)
                pl.when(own & crossed(r) & jnp.logical_not(by_ring))(
                    lambda: forward(8, slot, slot, parity, r, at(0, 0, 1 - xh, m))
                )

        lag = [by_half(v) for v in zip(*LAG_EVEN)]

        def step(t, carry):
            guarded(t - lag[0], first)
            guarded(t - lag[1], last)
            guarded(t - lag[2], sides)
            pl.when(t == 1)(pass_lhs)
            tile_step(t, jnp.maximum(lag[0], lag[1]), lag[2], True)
            return carry

        lax.fori_loop(0, steps + max(max(v[0], v[1] + 2, v[2] + 3) for v in LAG_EVEN), step, 0)
        pl.when(xl == 0)(lambda: drained(4, rows))
        settle(5, lambda half: R + sum(is_first(half)))
        settle(8, lambda half: sum(c * (3 - d) for c, d in zip(is_crossed(half), is_doubled(half))))

        @pl.when((y == 0) | (y == Y - 1))
        def _():
            settle(6, lambda half: 2 * sum(is_doubled(half)))
            settle(7, lambda half: 2 * sum(is_doubled(half)))

    @pl.when(core == 1)
    def _():
        def first(own, parity, r):
            arrived(0, parity, r)
            pl.when(own | marked(LAST_DOWN, 1, r))(
                lambda: forward(5, 0, 4, parity, r, at(-1, 0, xh, m))
            )
            pl.when(own & jnp.logical_not(marked(FIRST_DOWN, 3, r)))(
                lambda: forward(4, 0, 0, parity, r, at(0, 0, 1 - xh, m))
            )
            forward(6, 0, 4, parity, r, at(0, 0, xh, m - 1))
            pl.when(y > 0)(lambda: forward(8, 0, 1, parity, r, at(0, -1, xh, m)))
            pl.when(y == Y - 1)(lambda: forward(9, 0, 3, parity, r, at(0, 1, xh, m)))

        def last(own, parity, r):
            arrived(4, parity, r)

            @pl.when(own & (xl == 0))
            def _():
                forward(10, 4, 0, parity, r, at(0, 0, 0, 2))
                forward(11, 4, 0, parity, r, at(0, 0, 1, 2))

            pl.when(own & jnp.logical_not(marked(LAST_DOWN, 1, r)))(
                lambda: forward(7, 4, 4, parity, r, at(0, 0, 1 - xh, m))
            )
            pl.when(y < Y - 1)(lambda: forward(9, 4, 3, parity, r, at(0, 1, xh, m)))
            pl.when(y == 0)(lambda: forward(8, 4, 1, parity, r, at(0, -1, xh, m)))

        def relay(slot, own, parity, r):
            by_ring = doubled(r) & (side == slot)
            pl.when(jnp.logical_not(by_ring) & (own | jnp.logical_not(crossed(r))))(
                lambda: forward(12, slot, slot, parity, r, at(1, 0, xh, m - 1))
            )

        def toward(stream, slot, dy, own, parity, r):
            inner = (y == 1) | (y == 2)
            pl.when(inner & (own | jnp.logical_not(mid_crossed(r))))(
                lambda: forward(stream, slot, 2, parity, r, at(0, dy, xh, m))
            )

        def low_side(own, parity, r):
            arrived(1, parity, r)
            relay(1, own, parity, r)
            toward(14, 1, -1, own, parity, r)

        def high_side(own, parity, r):
            arrived(3, parity, r)
            relay(3, own, parity, r)
            toward(15, 3, 1, own, parity, r)

        def middle(own, parity, r):
            arrived(2, parity, r)
            relay(2, own, parity, r)
            pl.when(own & mid_crossed(r))(
                lambda: forward(13, 2, 2, parity, r, at(0, 0, 1 - xh, m))
            )

        lag = [by_half(v) for v in zip(*LAG_ODD)]

        def step(t, carry):
            guarded(t - lag[0], first)
            guarded(t - lag[1], last)
            guarded(t - lag[2], low_side)
            guarded(t - lag[3], high_side)
            guarded(t - lag[4], middle)
            pl.when(t == 1)(pass_lhs)
            tile_step(t, jnp.maximum(lag[0], lag[1]), lag[4], False)
            return carry

        lax.fori_loop(0, steps + max(max(*v, v[0] + 2, v[1] + 2, v[4] + 3) for v in LAG_ODD), step, 0)
        settle(4, lambda half: R - sum(is_first(half)))
        settle(5, lambda half: R + sum(is_last(half)))
        settle(7, lambda half: R - sum(is_last(half)))
        for stream in (6, 8, 9):
            drained(stream, pair)
        settle(10, lambda half: R * (1 - half))
        settle(11, lambda half: R * (1 - half))
        settle(12, lambda half: sum((3 - d) * (2 - c) for c, d in zip(is_crossed(half), is_doubled(half))))
        settle(13, lambda half: sum(is_mid(half)))

        @pl.when((y == 1) | (y == 2))
        def _():
            settle(14, lambda half: sum(2 - c for c in is_mid(half)))
            settle(15, lambda half: sum(2 - c for c in is_mid(half)))

    for copy in sent:
        copy.wait_send()
    lhs_copy(1, std, m, mate).wait_send()
    pl.when(m != 1)(lambda: lhs_copy(2, std, m, 1).wait_send())
    pl.when(m >= 2)(lambda: lhs_copy(3, std, m - 2, 5 - m).wait_send())
    pl.when(m != 0)(lambda: pltpu.make_async_copy(std, std, send.at[0]).wait())


def per_device(genotype, mask):
    circle = lax.axis_size("samples")
    rows, width = genotype.shape
    parts = lax.axis_size("snps")
    band = (circle // 2 + 1) * rows // parts
    total = width * parts
    z_size = circle // (2 * Y)

    call = (mask * (genotype + 1)).astype(jnp.bfloat16)

    def kernel(*refs):
        exchange_kernel(z_size, *refs)

    sums = pl.pallas_call(
        kernel,
        out_shape=jax.ShapeDtypeStruct((rows, band), jnp.float32),
        in_specs=[pl.BlockSpec(memory_space=pltpu.VMEM)],
        out_specs=pl.BlockSpec(memory_space=pltpu.VMEM),
        scratch_shapes=[
            pltpu.VMEM((rows, width), jnp.bfloat16),
            pltpu.VMEM((SLOTS * 2 * rows, total), jnp.bfloat16),
            pltpu.VMEM((rows, total), jnp.bfloat16),
            pltpu.VMEM((2 * Y, 8, width // 3), jnp.float32),
            pltpu.VMEM((z_size, 8, width // 3), jnp.float32),
            pltpu.SemaphoreType.DMA((SLOTS, 2, R)),
            pltpu.SemaphoreType.DMA((4, R)),
            pltpu.SemaphoreType.DMA((4,)),
            pltpu.SemaphoreType.DMA((2, max(z_size, 2 * Y))),
            pltpu.SemaphoreType.DMA((16,)),
            pltpu.SemaphoreType.DMA((2, max(z_size, 2 * Y))),
        ],
        compiler_params=pltpu.CompilerParams(
            collective_id=0, has_side_effects=True, vmem_limit_bytes=VMEM_MIB * 1024 * 1024
        ),
        cost_estimate=pl.CostEstimate(
            flops=2 * rows * band * total, bytes_accessed=rows * band * 4, transcendentals=0
        ),
    )(call)
    return sums


def solution(mesh):
    return jax.shard_map(
        per_device,
        mesh=mesh,
        in_specs=(P("samples", "snps"), P("samples", "snps")),
        out_specs=P("samples", "snps"),
        check_vma=False,
    )
```

```python
import jax
import jax.numpy as jnp
from jax import lax
from jax.experimental import pallas as pl
from jax.experimental.pallas import tpu as pltpu
from jax.sharding import PartitionSpec as P

MESH = pl.DeviceIdType.MESH
Y = 4
R = 16
SLOTS = 5
UNIT = 128
DOUBLED = (4, 3)
CROSSED = (3, 2)
MID_CROSSED = (0, 4)
FIRST_DOWN = (4, 3)
LAST_DOWN = (4, 4)
LAG_EVEN = ((1, 3, 13), (1, 3, 16))
LAG_ODD = ((0, 1, 2, 6, 8), (0, 2, 4, 4, 6))
VMEM_MIB = 30


def levels(allele_sum, observed_sum):
    frequency = (allele_sum + 1.0) / (2.0 * observed_sum + 2.0)
    spread = jnp.sqrt(2.0 * frequency * (1.0 - frequency))
    return [(dosage - 2.0 * frequency) / spread for dosage in (0.0, 1.0, 2.0)]


def exchange_kernel(
    z_size, call, out,
    std, slots, lhs, plane, column, recv, recv_piece, recv_row, recv_lhs, recv_count, send, send_count,
):
    rows, width = std.shape
    total = 4 * width
    pair = 2 * rows
    chunk = rows // R
    i = lax.axis_index("samples")
    m = lax.axis_index("snps")
    xh, q = i % 2, i // 2
    y, z = q % Y, q // Y
    core, xl = m % 2, m // 2
    mine, theirs = xh, 1 - xh
    band = out.shape[1]

    def at(dz, dy, half, member):
        zz = lax.rem(z + dz + z_size, z_size)
        yy = lax.rem(y + dy + Y, Y)
        return ((zz * Y + yy) * 2 + half, member)

    def span(slot, parity, r):
        return pl.ds(pl.multiple_of(slot * pair + parity * rows + r * chunk, chunk), chunk)

    def columns(member):
        return pl.ds(pl.multiple_of(member * width, width), width)

    def forward(stream, source, slot, parity, r, device):
        pltpu.make_async_remote_copy(
            src_ref=slots.at[span(source, parity, r)],
            dst_ref=slots.at[span(slot, parity, r)],
            send_sem=send.at[stream],
            recv_sem=recv.at[slot, parity, r],
            device_id=device,
            device_id_type=MESH,
        ).start()

    def arrived(slot, parity, r):
        pltpu.make_async_copy(
            slots.at[span(slot, parity, r)], slots.at[span(slot, parity, r)], recv.at[slot, parity, r]
        ).wait()

    def drained(stream, count):
        pltpu.make_async_copy(
            slots.at[pl.ds(0, count)], slots.at[pl.ds(0, count)], send.at[stream]
        ).wait()

    barrier = pltpu.get_barrier_semaphore()
    peers = []
    for dh in range(2):
        for dm in range(4):
            if dh or dm:
                peers.append(at(0, 0, lax.rem(xh + dh, 2), lax.rem(m + dm, 4)))
    for dz in (-1, 1):
        for c in range(2):
            peers.append(at(dz, 0, xh, xl * 2 + c))
    for dy in (-1, 1):
        peers.append(at(0, dy, xh, m))
    here = y * 2 + xh
    crowd = []
    for d in range(1, 2 * Y):
        other = lax.rem(here + d, 2 * Y)
        crowd.append((i - here + other, m))
    tower = [at(d, 0, xh, m) for d in range(1, z_size)]
    everyone = peers + crowd + tower
    for peer in everyone:
        pl.semaphore_signal(barrier, inc=1, device_id=peer, device_id_type=MESH)

    value = call[...].astype(jnp.float32)
    lanes = width // 3
    sums = (
        jnp.sum(jnp.maximum(value - 1.0, 0.0), axis=0, keepdims=True),
        jnp.sum(jnp.minimum(value, 1.0), axis=0, keepdims=True),
    )
    line = lax.broadcasted_iota(jnp.int32, (8, lanes), 0)
    packed = jnp.zeros((8, lanes), jnp.float32)
    for k in range(6):
        part = sums[k // 3][:, (k % 3) * lanes : (k % 3 + 1) * lanes]
        packed = jnp.where(line == k, part, packed)
    plane[here] = packed
    pl.semaphore_wait(barrier, len(everyone))

    def share(buffer, index, phase, devices, size):
        copies = [
            pltpu.make_async_remote_copy(
                src_ref=buffer.at[index],
                dst_ref=buffer.at[index],
                send_sem=send_count.at[phase, d],
                recv_sem=recv_count.at[phase, index],
                device_id=device,
                device_id_type=MESH,
            )
            for d, device in enumerate(devices)
        ]
        for copy in copies:
            copy.start()
        for d in range(1, size):
            source = lax.rem(index + d, size)
            pltpu.make_async_copy(
                buffer.at[source], buffer.at[source], recv_count.at[phase, source]
            ).wait()
        return copies

    sent = share(plane, here, 0, crowd, 2 * Y)
    column[z] = jnp.sum(plane[...], axis=0)
    sent += share(column, z, 1, tower, z_size)
    counts = jnp.sum(column[...], axis=0)
    alleles, observed = (
        jnp.concatenate([counts[3 * k + n : 3 * k + n + 1] for n in range(3)], axis=1) for k in range(2)
    )
    low, middle_level, high = levels(alleles, observed)
    seen = jnp.where(value == 1.0, low, jnp.where(value == 2.0, middle_level, high))
    standard = jnp.where(value == 0.0, 0.0, seen).astype(jnp.bfloat16)
    std[...] = standard
    own_rows = pl.ds(pl.multiple_of(xh * rows, rows), rows)

    @pl.when(m == 0)
    def _():
        slots[own_rows, 0:width] = standard

    for member in range(2, 4):
        @pl.when(m == member)
        def _():
            lhs[:, member * width : (member + 1) * width] = standard

    @pl.when(m != 0)
    def _():
        def piece(r, carry):
            pltpu.make_async_remote_copy(
                src_ref=std.at[pl.ds(pl.multiple_of(r * chunk, chunk), chunk)],
                dst_ref=slots.at[span(0, xh, r), columns(m)],
                send_sem=send.at[0],
                recv_sem=recv_piece.at[m, r],
                device_id=at(0, 0, xh, 0),
                device_id_type=MESH,
            ).start()
            return carry

        lax.fori_loop(0, R, piece, 0)

    def lhs_copy(stream, source, owner, member):
        return pltpu.make_async_remote_copy(
            src_ref=source,
            dst_ref=lhs.at[:, columns(owner)],
            send_sem=send.at[stream],
            recv_sem=recv_lhs.at[owner],
            device_id=at(0, 0, xh, member),
            device_id_type=MESH,
        )

    mate = jnp.where(m < 2, m + 2, 5 - m)
    lhs_copy(1, std, m, mate).start()

    def lhs_wait(owner):
        pltpu.make_async_copy(
            lhs.at[:, columns(owner)], lhs.at[:, columns(owner)], recv_lhs.at[owner]
        ).wait()

    def pass_lhs():
        @pl.when(m >= 2)
        def _():
            lhs_wait(m - 2)
            lhs_copy(3, lhs.at[:, columns(m - 2)], m - 2, 5 - m).start()

    def lhs_ready():
        @pl.when(m == 0)
        def _():
            lhs[...] = slots[own_rows, :]

        @pl.when(m == 1)
        def _():
            def row_wait(r, carry):
                row = lhs.at[pl.ds(pl.multiple_of(r * chunk, chunk), chunk)]
                pltpu.make_async_copy(row, row, recv_row.at[r]).wait()
                return carry

            lax.fori_loop(0, R, row_wait, 0)

        @pl.when(m >= 2)
        def _():
            lhs_wait(5 - m)
            lhs_wait(3 - m)

    begin = xh * 4 + m

    def product(unit, count):
        first = pl.multiple_of(unit * UNIT, UNIT)
        out[:, pl.ds(pl.multiple_of((unit - begin) * UNIT, UNIT), count * UNIT)] = lax.dot_general(
            lhs[...],
            slots[pl.ds(first, count * UNIT), :],
            (((1,), (1,)), ((), ())),
            preferred_element_type=jnp.float32,
        ) / total

    def tile(slot, parity, half):
        unit = slot * (pair // UNIT) + parity * (rows // UNIT) + half * 2
        low = unit - begin
        units = band // UNIT
        pl.when((low >= 0) & (low < units - 1))(lambda: product(unit, 2))
        pl.when(low == -1)(lambda: product(unit + 1, 1))
        pl.when(low == units - 1)(lambda: product(unit, 1))

    def by_half(values):
        return values[0] if values[0] == values[1] else jnp.where(xl == 0, values[0], values[1])

    def marked(shares, shift, r):
        return lax.rem(r + shift, 4) < by_half(shares)

    def doubled(r):
        return marked(DOUBLED, 0, r)

    def crossed(r):
        return marked(CROSSED, 1, r)

    def mid_crossed(r):
        return marked(MID_CROSSED, 2, r)

    def guarded(n, body):
        @pl.when((n >= 0) & (n < 2 * R))
        def _():
            own = n < R
            body(own, jnp.where(own, mine, theirs), lax.rem(n, R))

    def both_ways(source, parity, r):
        forward(6, source, 3, parity, r, at(0, 1, xh, m))
        forward(7, source, 1, parity, r, at(0, -1, xh, m))

    def tiles_of(k, group, start=0, stop=4):
        j, phase = lax.rem(k, R // 2), k // (R // 2)

        @pl.when((k >= 0) & (phase >= start) & (phase < stop) & (j < len(group)))
        def _():
            slot = jnp.int32(group[-1])
            for place, value in enumerate(group[:-1]):
                slot = jnp.where(j == place, value, slot)
            tile(slot, jnp.where(phase < 2, mine, theirs), lax.rem(phase, 2))

    def tile_step(t, early, late):
        ready = early + R
        pl.when(t == ready)(lhs_ready)
        tiles_of(t - early - R // 2, (0, 4), start=1)
        tiles_of(t - ready - 2, (0, 4), stop=1)
        tiles_of(t - late - R // 2, (1, 3, 2), start=1)
        tiles_of(t - jnp.maximum(late + R // 2, ready + 4), (1, 3, 2), stop=1)

    def settle(stream, count):
        for half in range(2):
            if count(half):
                pl.when(xl == half)(lambda: drained(stream, chunk * count(half)))

    def tally(shares, shift):
        return lambda half: [int((r + shift) % 4 < shares[half]) for r in range(R)]

    is_doubled, is_crossed, is_mid = tally(DOUBLED, 0), tally(CROSSED, 1), tally(MID_CROSSED, 2)
    is_first, is_last = tally(FIRST_DOWN, 3), tally(LAST_DOWN, 1)
    steps = 2 * R
    side = jnp.where(y < 2, 3, 1)

    @pl.when(core == 0)
    def _():
        def first(own, parity, r):
            @pl.when(own & (xl == 0))
            def _():
                for member in range(1, 4):
                    pltpu.make_async_copy(
                        slots.at[span(0, xh, r), columns(member)],
                        slots.at[span(0, xh, r), columns(member)],
                        recv_piece.at[member, r],
                    ).wait()
                forward(4, 0, 0, mine, r, at(0, 0, 1 - xh, m))
                pltpu.make_async_remote_copy(
                    src_ref=slots.at[span(0, mine, r)],
                    dst_ref=lhs.at[pl.ds(pl.multiple_of(r * chunk, chunk), chunk)],
                    send_sem=send.at[2],
                    recv_sem=recv_row.at[r],
                    device_id=at(0, 0, xh, 1),
                    device_id_type=MESH,
                ).start()

            @pl.when(jnp.logical_not(own & (xl == 0)))
            def _():
                arrived(0, parity, r)

            pl.when(own | marked(FIRST_DOWN, 3, r))(
                lambda: forward(5, 0, 0, parity, r, at(-1, 0, xh, m + 1))
            )
            pl.when((y == Y - 1) & doubled(r))(lambda: both_ways(0, parity, r))

        def last(own, parity, r):
            arrived(4, parity, r)
            pl.when((y == 0) & doubled(r))(lambda: both_ways(4, parity, r))

        def sides(own, parity, r):
            for slot in (1, 3, 2):
                arrived(slot, parity, r)
                by_ring = doubled(r) & (side == slot)
                pl.when(own & crossed(r) & jnp.logical_not(by_ring))(
                    lambda: forward(8, slot, slot, parity, r, at(0, 0, 1 - xh, m))
                )

        lag = [by_half(v) for v in zip(*LAG_EVEN)]

        def step(t, carry):
            guarded(t - lag[0], first)
            guarded(t - lag[1], last)
            guarded(t - lag[2], sides)
            pl.when(t == 1)(pass_lhs)
            tile_step(t, jnp.maximum(lag[0], lag[1]), lag[2])
            return carry

        lax.fori_loop(0, steps + max(max(v[0], v[1] + 2, v[2] + 3) for v in LAG_EVEN), step, 0)
        pl.when(xl == 0)(lambda: drained(4, rows))
        pl.when(xl == 0)(lambda: drained(2, rows))
        settle(5, lambda half: R + sum(is_first(half)))
        settle(8, lambda half: sum(c * (3 - d) for c, d in zip(is_crossed(half), is_doubled(half))))

        @pl.when((y == 0) | (y == Y - 1))
        def _():
            settle(6, lambda half: 2 * sum(is_doubled(half)))
            settle(7, lambda half: 2 * sum(is_doubled(half)))

    @pl.when(core == 1)
    def _():
        def first(own, parity, r):
            arrived(0, parity, r)
            pl.when(own | marked(LAST_DOWN, 1, r))(
                lambda: forward(5, 0, 4, parity, r, at(-1, 0, xh, m))
            )
            pl.when(own & jnp.logical_not(marked(FIRST_DOWN, 3, r)))(
                lambda: forward(4, 0, 0, parity, r, at(0, 0, 1 - xh, m))
            )
            forward(6, 0, 4, parity, r, at(0, 0, xh, m - 1))
            pl.when(y > 0)(lambda: forward(8, 0, 1, parity, r, at(0, -1, xh, m)))
            pl.when(y == Y - 1)(lambda: forward(9, 0, 3, parity, r, at(0, 1, xh, m)))

        def last(own, parity, r):
            arrived(4, parity, r)

            @pl.when(own & (xl == 0))
            def _():
                forward(10, 4, 0, parity, r, at(0, 0, 0, 2))
                forward(11, 4, 0, parity, r, at(0, 0, 1, 2))

            pl.when(own & jnp.logical_not(marked(LAST_DOWN, 1, r)))(
                lambda: forward(7, 4, 4, parity, r, at(0, 0, 1 - xh, m))
            )
            pl.when(y < Y - 1)(lambda: forward(9, 4, 3, parity, r, at(0, 1, xh, m)))
            pl.when(y == 0)(lambda: forward(8, 4, 1, parity, r, at(0, -1, xh, m)))

        def relay(slot, own, parity, r):
            by_ring = doubled(r) & (side == slot)
            pl.when(jnp.logical_not(by_ring) & (own | jnp.logical_not(crossed(r))))(
                lambda: forward(12, slot, slot, parity, r, at(1, 0, xh, m - 1))
            )

        def toward(stream, slot, dy, own, parity, r):
            inner = (y == 1) | (y == 2)
            pl.when(inner & (own | jnp.logical_not(mid_crossed(r))))(
                lambda: forward(stream, slot, 2, parity, r, at(0, dy, xh, m))
            )

        def low_side(own, parity, r):
            arrived(1, parity, r)
            relay(1, own, parity, r)
            toward(14, 1, -1, own, parity, r)

        def high_side(own, parity, r):
            arrived(3, parity, r)
            relay(3, own, parity, r)
            toward(15, 3, 1, own, parity, r)

        def middle(own, parity, r):
            arrived(2, parity, r)
            relay(2, own, parity, r)
            pl.when(own & mid_crossed(r))(
                lambda: forward(13, 2, 2, parity, r, at(0, 0, 1 - xh, m))
            )

        lag = [by_half(v) for v in zip(*LAG_ODD)]

        def step(t, carry):
            guarded(t - lag[0], first)
            guarded(t - lag[1], last)
            guarded(t - lag[2], low_side)
            guarded(t - lag[3], high_side)
            guarded(t - lag[4], middle)
            pl.when(t == 1)(pass_lhs)
            tile_step(t, jnp.maximum(lag[0], lag[1]), lag[4])
            return carry

        lax.fori_loop(0, steps + max(max(*v, v[0] + 2, v[1] + 2, v[4] + 3) for v in LAG_ODD), step, 0)
        settle(4, lambda half: R - sum(is_first(half)))
        settle(5, lambda half: R + sum(is_last(half)))
        settle(7, lambda half: R - sum(is_last(half)))
        for stream in (6, 8, 9):
            drained(stream, pair)
        settle(10, lambda half: R * (1 - half))
        settle(11, lambda half: R * (1 - half))
        settle(12, lambda half: sum((3 - d) * (2 - c) for c, d in zip(is_crossed(half), is_doubled(half))))
        settle(13, lambda half: sum(is_mid(half)))

        @pl.when((y == 1) | (y == 2))
        def _():
            settle(14, lambda half: sum(2 - c for c in is_mid(half)))
            settle(15, lambda half: sum(2 - c for c in is_mid(half)))

    for copy in sent:
        copy.wait_send()
    lhs_copy(1, std, m, mate).wait_send()
    pl.when(m >= 2)(lambda: lhs_copy(3, std, m - 2, 5 - m).wait_send())
    pl.when(m != 0)(lambda: pltpu.make_async_copy(std, std, send.at[0]).wait())


def per_device(genotype, mask):
    circle = lax.axis_size("samples")
    rows, width = genotype.shape
    parts = lax.axis_size("snps")
    band = (circle // 2 + 1) * rows // parts
    total = width * parts
    z_size = circle // (2 * Y)

    call = (mask * (genotype + 1)).astype(jnp.bfloat16)

    def kernel(*refs):
        exchange_kernel(z_size, *refs)

    sums = pl.pallas_call(
        kernel,
        out_shape=jax.ShapeDtypeStruct((rows, band), jnp.float32),
        in_specs=[pl.BlockSpec(memory_space=pltpu.VMEM)],
        out_specs=pl.BlockSpec(memory_space=pltpu.VMEM),
        scratch_shapes=[
            pltpu.VMEM((rows, width), jnp.bfloat16),
            pltpu.VMEM((SLOTS * 2 * rows, total), jnp.bfloat16),
            pltpu.VMEM((rows, total), jnp.bfloat16),
            pltpu.VMEM((2 * Y, 8, width // 3), jnp.float32),
            pltpu.VMEM((z_size, 8, width // 3), jnp.float32),
            pltpu.SemaphoreType.DMA((SLOTS, 2, R)),
            pltpu.SemaphoreType.DMA((4, R)),
            pltpu.SemaphoreType.DMA((R,)),
            pltpu.SemaphoreType.DMA((4,)),
            pltpu.SemaphoreType.DMA((2, max(z_size, 2 * Y))),
            pltpu.SemaphoreType.DMA((16,)),
            pltpu.SemaphoreType.DMA((2, max(z_size, 2 * Y))),
        ],
        compiler_params=pltpu.CompilerParams(
            collective_id=0, has_side_effects=True, vmem_limit_bytes=VMEM_MIB * 1024 * 1024
        ),
        cost_estimate=pl.CostEstimate(
            flops=2 * rows * band * total, bytes_accessed=rows * band * 4, transcendentals=0
        ),
    )(call)
    return sums


def solution(mesh):
    return jax.shard_map(
        per_device,
        mesh=mesh,
        in_specs=(P("samples", "snps"), P("samples", "snps")),
        out_specs=P("samples", "snps"),
        check_vma=False,
    )
```

```python
import jax
import jax.numpy as jnp
from jax import lax
from jax.experimental import pallas as pl
from jax.experimental.pallas import tpu as pltpu
from jax.sharding import PartitionSpec as P

MESH = pl.DeviceIdType.MESH
Y = 4
R = 16
SLOTS = 5
UNIT = 128
DOUBLED = (4, 3)
CROSSED = (2, 2)
MID_CROSSED = (0, 4)
FIRST_DOWN = (4, 3)
LAST_DOWN = (4, 4)
LAG_EVEN = ((0, 2, 12), (0, 2, 15))
LAG_ODD = ((0, 1, 2, 4, 6), (0, 2, 4, 4, 6))
VMEM_MIB = 30


def levels(allele_sum, observed_sum):
    frequency = (allele_sum + 1.0) / (2.0 * observed_sum + 2.0)
    spread = jnp.sqrt(2.0 * frequency * (1.0 - frequency))
    return [(dosage - 2.0 * frequency) / spread for dosage in (0.0, 1.0, 2.0)]


def exchange_kernel(
    z_size, call, out,
    std, slots, lhs, plane, column, recv, recv_piece, recv_row, recv_lhs, recv_count, send, send_count,
):
    rows, width = std.shape
    total = 4 * width
    pair = 2 * rows
    chunk = rows // R
    i = lax.axis_index("samples")
    m = lax.axis_index("snps")
    xh, q = i % 2, i // 2
    y, z = q % Y, q // Y
    core, xl = m % 2, m // 2
    mine, theirs = xh, 1 - xh
    band = out.shape[1]

    def at(dz, dy, half, member):
        zz = lax.rem(z + dz + z_size, z_size)
        yy = lax.rem(y + dy + Y, Y)
        return ((zz * Y + yy) * 2 + half, member)

    def span(slot, parity, r):
        return pl.ds(pl.multiple_of(slot * pair + parity * rows + r * chunk, chunk), chunk)

    def columns(member):
        return pl.ds(pl.multiple_of(member * width, width), width)

    def forward(stream, source, slot, parity, r, device):
        pltpu.make_async_remote_copy(
            src_ref=slots.at[span(source, parity, r)],
            dst_ref=slots.at[span(slot, parity, r)],
            send_sem=send.at[stream],
            recv_sem=recv.at[slot, parity, r],
            device_id=device,
            device_id_type=MESH,
        ).start()

    def arrived(slot, parity, r):
        pltpu.make_async_copy(
            slots.at[span(slot, parity, r)], slots.at[span(slot, parity, r)], recv.at[slot, parity, r]
        ).wait()

    def drained(stream, count):
        pltpu.make_async_copy(
            slots.at[pl.ds(0, count)], slots.at[pl.ds(0, count)], send.at[stream]
        ).wait()

    barrier = pltpu.get_barrier_semaphore()
    peers = []
    for dh in range(2):
        for dm in range(4):
            if dh or dm:
                peers.append(at(0, 0, lax.rem(xh + dh, 2), lax.rem(m + dm, 4)))
    for dz in (-1, 1):
        for c in range(2):
            peers.append(at(dz, 0, xh, xl * 2 + c))
    for dy in (-1, 1):
        peers.append(at(0, dy, xh, m))
    here = y * 2 + xh
    crowd = []
    for d in range(1, 2 * Y):
        other = lax.rem(here + d, 2 * Y)
        crowd.append((i - here + other, m))
    tower = [at(d, 0, xh, m) for d in range(1, z_size)]
    everyone = peers + crowd + tower
    for peer in everyone:
        pl.semaphore_signal(barrier, inc=1, device_id=peer, device_id_type=MESH)

    value = call[...].astype(jnp.float32)
    lanes = width // 3
    sums = (
        jnp.sum(jnp.maximum(value - 1.0, 0.0), axis=0, keepdims=True),
        jnp.sum(jnp.minimum(value, 1.0), axis=0, keepdims=True),
    )
    line = lax.broadcasted_iota(jnp.int32, (8, lanes), 0)
    packed = jnp.zeros((8, lanes), jnp.float32)
    for k in range(6):
        part = sums[k // 3][:, (k % 3) * lanes : (k % 3 + 1) * lanes]
        packed = jnp.where(line == k, part, packed)
    plane[here] = packed
    pl.semaphore_wait(barrier, len(everyone))

    def share(buffer, index, phase, devices, size):
        copies = [
            pltpu.make_async_remote_copy(
                src_ref=buffer.at[index],
                dst_ref=buffer.at[index],
                send_sem=send_count.at[phase, d],
                recv_sem=recv_count.at[phase, index],
                device_id=device,
                device_id_type=MESH,
            )
            for d, device in enumerate(devices)
        ]
        for copy in copies:
            copy.start()
        for d in range(1, size):
            source = lax.rem(index + d, size)
            pltpu.make_async_copy(
                buffer.at[source], buffer.at[source], recv_count.at[phase, source]
            ).wait()
        return copies

    sent = share(plane, here, 0, crowd, 2 * Y)
    column[z] = jnp.sum(plane[...], axis=0)
    sent += share(column, z, 1, tower, z_size)
    counts = jnp.sum(column[...], axis=0)
    alleles, observed = (
        jnp.concatenate([counts[3 * k + n : 3 * k + n + 1] for n in range(3)], axis=1) for k in range(2)
    )
    low, middle_level, high = levels(alleles, observed)
    seen = jnp.where(value == 1.0, low, jnp.where(value == 2.0, middle_level, high))
    standard = jnp.where(value == 0.0, 0.0, seen).astype(jnp.bfloat16)
    std[...] = standard
    own_rows = pl.ds(pl.multiple_of(xh * rows, rows), rows)

    @pl.when(m == 0)
    def _():
        slots[own_rows, 0:width] = standard

    for member in range(2, 4):
        @pl.when(m == member)
        def _():
            lhs[:, member * width : (member + 1) * width] = standard

    @pl.when(m != 0)
    def _():
        def piece(r, carry):
            pltpu.make_async_remote_copy(
                src_ref=std.at[pl.ds(pl.multiple_of(r * chunk, chunk), chunk)],
                dst_ref=slots.at[span(0, xh, r), columns(m)],
                send_sem=send.at[0],
                recv_sem=recv_piece.at[m, r],
                device_id=at(0, 0, xh, 0),
                device_id_type=MESH,
            ).start()
            return carry

        lax.fori_loop(0, R, piece, 0)

    def lhs_copy(stream, source, owner, member):
        return pltpu.make_async_remote_copy(
            src_ref=source,
            dst_ref=lhs.at[:, columns(owner)],
            send_sem=send.at[stream],
            recv_sem=recv_lhs.at[owner],
            device_id=at(0, 0, xh, member),
            device_id_type=MESH,
        )

    mate = jnp.where(m < 2, m + 2, 5 - m)
    lhs_copy(1, std, m, mate).start()

    def lhs_wait(owner):
        pltpu.make_async_copy(
            lhs.at[:, columns(owner)], lhs.at[:, columns(owner)], recv_lhs.at[owner]
        ).wait()

    def pass_lhs():
        @pl.when(m >= 2)
        def _():
            lhs_wait(m - 2)
            lhs_copy(3, lhs.at[:, columns(m - 2)], m - 2, 5 - m).start()

    def lhs_ready():
        @pl.when(m == 0)
        def _():
            lhs[...] = slots[own_rows, :]

        @pl.when(m == 1)
        def _():
            def row_wait(r, carry):
                row = lhs.at[pl.ds(pl.multiple_of(r * chunk, chunk), chunk)]
                pltpu.make_async_copy(row, row, recv_row.at[r]).wait()
                return carry

            lax.fori_loop(0, R, row_wait, 0)

        @pl.when(m >= 2)
        def _():
            lhs_wait(5 - m)
            lhs_wait(3 - m)

    begin = xh * 4 + m

    def product(unit, count):
        first = pl.multiple_of(unit * UNIT, UNIT)
        out[:, pl.ds(pl.multiple_of((unit - begin) * UNIT, UNIT), count * UNIT)] = lax.dot_general(
            lhs[...],
            slots[pl.ds(first, count * UNIT), :],
            (((1,), (1,)), ((), ())),
            preferred_element_type=jnp.float32,
        ) / total

    def tile(slot, parity, half):
        unit = slot * (pair // UNIT) + parity * (rows // UNIT) + half * 2
        low = unit - begin
        units = band // UNIT
        pl.when((low >= 0) & (low < units - 1))(lambda: product(unit, 2))
        pl.when(low == -1)(lambda: product(unit + 1, 1))
        pl.when(low == units - 1)(lambda: product(unit, 1))

    def by_half(values):
        return values[0] if values[0] == values[1] else jnp.where(xl == 0, values[0], values[1])

    def marked(shares, shift, r):
        return lax.rem(r + shift, 4) < by_half(shares)

    def doubled(r):
        return marked(DOUBLED, 0, r)

    def crossed(r):
        return marked(CROSSED, 1, r)

    def mid_crossed(r):
        return marked(MID_CROSSED, 2, r)

    def guarded(n, body):
        @pl.when((n >= 0) & (n < 2 * R))
        def _():
            own = n < R
            body(own, jnp.where(own, mine, theirs), lax.rem(n, R))

    def both_ways(source, parity, r):
        forward(6, source, 3, parity, r, at(0, 1, xh, m))
        forward(7, source, 1, parity, r, at(0, -1, xh, m))

    def tiles_of(k, group, start=0, stop=4):
        j, phase = lax.rem(k, R // 2), k // (R // 2)

        @pl.when((k >= 0) & (phase >= start) & (phase < stop) & (j < len(group)))
        def _():
            slot = jnp.int32(group[-1])
            for place, value in enumerate(group[:-1]):
                slot = jnp.where(j == place, value, slot)
            tile(slot, jnp.where(phase < 2, mine, theirs), lax.rem(phase, 2))

    def tile_step(t, early, late):
        ready = early + R
        pl.when(t == ready)(lhs_ready)
        tiles_of(t - early - R // 2, (0, 4), start=1)
        tiles_of(t - ready - 2, (0, 4), stop=1)
        tiles_of(t - late - R // 2, (1, 3, 2), start=1)
        tiles_of(t - jnp.maximum(late + R // 2, ready + 4), (1, 3, 2), stop=1)

    def settle(stream, count):
        for half in range(2):
            if count(half):
                pl.when(xl == half)(lambda: drained(stream, chunk * count(half)))

    def tally(shares, shift):
        return lambda half: [int((r + shift) % 4 < shares[half]) for r in range(R)]

    is_doubled, is_crossed, is_mid = tally(DOUBLED, 0), tally(CROSSED, 1), tally(MID_CROSSED, 2)
    is_first, is_last = tally(FIRST_DOWN, 3), tally(LAST_DOWN, 1)
    steps = 2 * R
    side = jnp.where(y < 2, 3, 1)

    @pl.when(core == 0)
    def _():
        def first(own, parity, r):
            @pl.when(own & (xl == 0))
            def _():
                for member in range(1, 4):
                    pltpu.make_async_copy(
                        slots.at[span(0, xh, r), columns(member)],
                        slots.at[span(0, xh, r), columns(member)],
                        recv_piece.at[member, r],
                    ).wait()
                forward(4, 0, 0, mine, r, at(0, 0, 1 - xh, m))
                pltpu.make_async_remote_copy(
                    src_ref=slots.at[span(0, mine, r)],
                    dst_ref=lhs.at[pl.ds(pl.multiple_of(r * chunk, chunk), chunk)],
                    send_sem=send.at[2],
                    recv_sem=recv_row.at[r],
                    device_id=at(0, 0, xh, 1),
                    device_id_type=MESH,
                ).start()

            @pl.when(jnp.logical_not(own & (xl == 0)))
            def _():
                arrived(0, parity, r)

            pl.when(own | marked(FIRST_DOWN, 3, r))(
                lambda: forward(5, 0, 0, parity, r, at(-1, 0, xh, m + 1))
            )
            pl.when((y == Y - 1) & doubled(r))(lambda: both_ways(0, parity, r))

        def last(own, parity, r):
            arrived(4, parity, r)
            pl.when((y == 0) & doubled(r))(lambda: both_ways(4, parity, r))

        def sides(own, parity, r):
            for slot in (1, 3, 2):
                arrived(slot, parity, r)
                by_ring = doubled(r) & (side == slot)
                pl.when(own & crossed(r) & jnp.logical_not(by_ring))(
                    lambda: forward(8, slot, slot, parity, r, at(0, 0, 1 - xh, m))
                )

        lag = [by_half(v) for v in zip(*LAG_EVEN)]

        def step(t, carry):
            guarded(t - lag[0], first)
            guarded(t - lag[1], last)
            guarded(t - lag[2], sides)
            pl.when(t == 1)(pass_lhs)
            tile_step(t, jnp.maximum(lag[0], lag[1]), lag[2])
            return carry

        lax.fori_loop(0, steps + max(max(v[0], v[1] + 2, v[2] + 3) for v in LAG_EVEN), step, 0)
        pl.when(xl == 0)(lambda: drained(4, rows))
        pl.when(xl == 0)(lambda: drained(2, rows))
        settle(5, lambda half: R + sum(is_first(half)))
        settle(8, lambda half: sum(c * (3 - d) for c, d in zip(is_crossed(half), is_doubled(half))))

        @pl.when((y == 0) | (y == Y - 1))
        def _():
            settle(6, lambda half: 2 * sum(is_doubled(half)))
            settle(7, lambda half: 2 * sum(is_doubled(half)))

    @pl.when(core == 1)
    def _():
        def first(own, parity, r):
            arrived(0, parity, r)
            pl.when(own | marked(LAST_DOWN, 1, r))(
                lambda: forward(5, 0, 4, parity, r, at(-1, 0, xh, m))
            )
            pl.when(own & jnp.logical_not(marked(FIRST_DOWN, 3, r)))(
                lambda: forward(4, 0, 0, parity, r, at(0, 0, 1 - xh, m))
            )
            forward(6, 0, 4, parity, r, at(0, 0, xh, m - 1))
            pl.when(y > 0)(lambda: forward(8, 0, 1, parity, r, at(0, -1, xh, m)))
            pl.when(y == Y - 1)(lambda: forward(9, 0, 3, parity, r, at(0, 1, xh, m)))

        def last(own, parity, r):
            arrived(4, parity, r)

            @pl.when(own & (xl == 0))
            def _():
                forward(10, 4, 0, parity, r, at(0, 0, 0, 2))
                forward(11, 4, 0, parity, r, at(0, 0, 1, 2))

            pl.when(own & jnp.logical_not(marked(LAST_DOWN, 1, r)))(
                lambda: forward(7, 4, 4, parity, r, at(0, 0, 1 - xh, m))
            )
            pl.when(y < Y - 1)(lambda: forward(9, 4, 3, parity, r, at(0, 1, xh, m)))
            pl.when(y == 0)(lambda: forward(8, 4, 1, parity, r, at(0, -1, xh, m)))

        def relay(slot, own, parity, r):
            by_ring = doubled(r) & (side == slot)
            pl.when(jnp.logical_not(by_ring) & (own | jnp.logical_not(crossed(r))))(
                lambda: forward(12, slot, slot, parity, r, at(1, 0, xh, m - 1))
            )

        def toward(stream, slot, dy, own, parity, r):
            inner = (y == 1) | (y == 2)
            pl.when(inner & (own | jnp.logical_not(mid_crossed(r))))(
                lambda: forward(stream, slot, 2, parity, r, at(0, dy, xh, m))
            )

        def low_side(own, parity, r):
            arrived(1, parity, r)
            relay(1, own, parity, r)
            toward(14, 1, -1, own, parity, r)

        def high_side(own, parity, r):
            arrived(3, parity, r)
            relay(3, own, parity, r)
            toward(15, 3, 1, own, parity, r)

        def middle(own, parity, r):
            arrived(2, parity, r)
            relay(2, own, parity, r)
            pl.when(own & mid_crossed(r))(
                lambda: forward(13, 2, 2, parity, r, at(0, 0, 1 - xh, m))
            )

        lag = [by_half(v) for v in zip(*LAG_ODD)]

        def step(t, carry):
            guarded(t - lag[0], first)
            guarded(t - lag[1], last)
            guarded(t - lag[2], low_side)
            guarded(t - lag[3], high_side)
            guarded(t - lag[4], middle)
            pl.when(t == 1)(pass_lhs)
            tile_step(t, jnp.maximum(lag[0], lag[1]), lag[4])
            return carry

        lax.fori_loop(0, steps + max(max(*v, v[0] + 2, v[1] + 2, v[4] + 3) for v in LAG_ODD), step, 0)
        settle(4, lambda half: R - sum(is_first(half)))
        settle(5, lambda half: R + sum(is_last(half)))
        settle(7, lambda half: R - sum(is_last(half)))
        for stream in (6, 8, 9):
            drained(stream, pair)
        settle(10, lambda half: R * (1 - half))
        settle(11, lambda half: R * (1 - half))
        settle(12, lambda half: sum((3 - d) * (2 - c) for c, d in zip(is_crossed(half), is_doubled(half))))
        settle(13, lambda half: sum(is_mid(half)))

        @pl.when((y == 1) | (y == 2))
        def _():
            settle(14, lambda half: sum(2 - c for c in is_mid(half)))
            settle(15, lambda half: sum(2 - c for c in is_mid(half)))

    for copy in sent:
        copy.wait_send()
    lhs_copy(1, std, m, mate).wait_send()
    pl.when(m >= 2)(lambda: lhs_copy(3, std, m - 2, 5 - m).wait_send())
    pl.when(m != 0)(lambda: pltpu.make_async_copy(std, std, send.at[0]).wait())


def per_device(genotype, mask):
    circle = lax.axis_size("samples")
    rows, width = genotype.shape
    parts = lax.axis_size("snps")
    band = (circle // 2 + 1) * rows // parts
    total = width * parts
    z_size = circle // (2 * Y)

    call = (mask * (genotype + 1)).astype(jnp.bfloat16)

    def kernel(*refs):
        exchange_kernel(z_size, *refs)

    sums = pl.pallas_call(
        kernel,
        out_shape=jax.ShapeDtypeStruct((rows, band), jnp.float32),
        in_specs=[pl.BlockSpec(memory_space=pltpu.VMEM)],
        out_specs=pl.BlockSpec(memory_space=pltpu.VMEM),
        scratch_shapes=[
            pltpu.VMEM((rows, width), jnp.bfloat16),
            pltpu.VMEM((SLOTS * 2 * rows, total), jnp.bfloat16),
            pltpu.VMEM((rows, total), jnp.bfloat16),
            pltpu.VMEM((2 * Y, 8, width // 3), jnp.float32),
            pltpu.VMEM((z_size, 8, width // 3), jnp.float32),
            pltpu.SemaphoreType.DMA((SLOTS, 2, R)),
            pltpu.SemaphoreType.DMA((4, R)),
            pltpu.SemaphoreType.DMA((R,)),
            pltpu.SemaphoreType.DMA((4,)),
            pltpu.SemaphoreType.DMA((2, max(z_size, 2 * Y))),
            pltpu.SemaphoreType.DMA((16,)),
            pltpu.SemaphoreType.DMA((2, max(z_size, 2 * Y))),
        ],
        compiler_params=pltpu.CompilerParams(
            collective_id=0, has_side_effects=True, vmem_limit_bytes=VMEM_MIB * 1024 * 1024
        ),
        cost_estimate=pl.CostEstimate(
            flops=2 * rows * band * total, bytes_accessed=rows * band * 4, transcendentals=0
        ),
    )(call)
    return sums


def solution(mesh):
    return jax.shard_map(
        per_device,
        mesh=mesh,
        in_specs=(P("samples", "snps"), P("samples", "snps")),
        out_specs=P("samples", "snps"),
        check_vma=False,
    )
```
